128 devices in a mesh: sub: 8 (over z, core), ma: 16 (over y, x).
Axes of the slice: x: 4, y: 4, z: 4, core: 2. Of those that a mesh axis runs over, the one named last changes fastest.
Arguments:
- forcing: float32 [2, 512, 2, 128, 512], P(None, 'sub', None, 'ma'), may hold values from -24 to 24
- slot_wavenumber: int32 [128], P('ma'), may hold values from 0 to 511, as said below
- inverse: float32 [8, 2, 64, 64, 512], P('sub'), may hold values from -2 to 2
- edge_weights: float32 [8, 2, 64], P('sub'), may hold values from -2908 to 2908, as said below
Outputs:
- transform_field: float32 [2, 512, 2, 128, 512], P(None, ('sub', 'ma'))
The draws below stay inside these ranges and needn't reach their ends.
Inputs may be any that keep to these rules, and one draw needn't show every extreme that they name: `slot_wavenumber`: each device's slots hold 4 pairs: slots 2j and 2j + 1 carry a wavenumber m below 256 and 511 - m, in that order; no wavenumber appears twice. `edge_weights`: together with inverse it makes every row of the interface system strictly diagonally dominant with a positive diagonal.
All inputs are finite; a program needn't handle non-finite values.
Results may differ from the reference program's by a relative error of at most 0.0003.
Values sent between devices are 32-bit elements; how exact they have to be, the bound alone decides.
A program may use at most 192 MiB of HBM per device.

```python
import math
import jax
import jax.numpy as jnp
from jax import lax

P_SIZE = 64
L = 512
FIELDS = 2
NSUB = 8
MTOT = 128
NR = 512


def shell_radius(key):
    widths = jax.random.uniform(jax.random.fold_in(key, 11), (NSUB,), jnp.float32, 1.0, 2.0)
    widths = 0.65 * widths / jnp.sum(widths)
    starts = 0.35 + jnp.cumsum(widths) - widths
    spacing = jnp.arange(P_SIZE, dtype=jnp.float32) / (P_SIZE - 1)
    return (starts[:, None] + widths[:, None] * spacing[None, :], widths)


def draw_slot_wavenumber(key, part):
    halfway = L // 2
    chosen = jax.random.permutation(jax.random.fold_in(key, 21), halfway)[:MTOT // 2]
    paired = jnp.stack([chosen, L - 1 - chosen], axis=1).reshape(MTOT)
    return paired.astype(jnp.int32)


def draw_edge_weights(key, part):
    radius, widths = shell_radius(key)
    step_size = widths / (P_SIZE - 1)
    lower_row = jnp.zeros((NSUB, P_SIZE), jnp.float32)
    lower_row = lower_row.at[:, 0].set(-1.5 / step_size).at[:, 1].set(2.0 / step_size).at[:, 2].set(-0.5 / step_size)
    upper_row = jnp.zeros((NSUB, P_SIZE), jnp.float32)
    upper_row = upper_row.at[:, P_SIZE - 1].set(1.5 / step_size).at[:, P_SIZE - 2].set(-2.0 / step_size).at[:, P_SIZE - 3].set(0.5 / step_size)
    return jnp.stack([lower_row, upper_row], axis=1)


def draw_inverse(key, part):
    radius, widths = shell_radius(key)
    field_scale = jnp.exp(jax.random.uniform(jax.random.fold_in(key, 12), (FIELDS,), jnp.float32, math.log(0.05), math.log(0.5)))
    degree_scale = jnp.exp(jax.random.uniform(jax.random.fold_in(key, 13), (FIELDS, L), jnp.float32, 0.0, math.log(3.0)))
    strength = (field_scale[:, None] * degree_scale)[None, :, :, None]
    degree = jnp.arange(L, dtype=jnp.float32)
    angular = degree * (degree + 1.0)
    inner = radius[:, 1:-1]
    below_gap = radius[:, 1:-1] - radius[:, :-2]
    above_gap = radius[:, 2:] - radius[:, 1:-1]
    spans = below_gap + above_gap
    sub_coef = 2.0 / (below_gap * spans) - 2.0 / (inner * spans)
    sup_coef = 2.0 / (above_gap * spans) + 2.0 / (inner * spans)
    mid_coef = 2.0 / (below_gap * above_gap)
    lower_band = -strength * sub_coef[:, None, None, :]
    upper_band = -strength * sup_coef[:, None, None, :]
    main_band = 1.0 + strength * (mid_coef[:, None, None, :] + angular[None, None, :, None] / (inner[:, None, None, :] * inner[:, None, None, :]))
    edges = ((0, 0), (0, 0), (0, 0), (1, 1))
    lower_band = jnp.pad(lower_band, edges)
    upper_band = jnp.pad(upper_band, edges)
    main_band = jnp.pad(main_band, edges, constant_values=1.0)
    bands = (jnp.moveaxis(lower_band, -1, 0), jnp.moveaxis(main_band, -1, 0), jnp.moveaxis(upper_band, -1, 0), jnp.eye(P_SIZE, dtype=jnp.float32))

    def forward(state_pair, inputs):
        prior_ratio, prior_value = state_pair
        sub_entry, main_entry, sup_entry, unit_row = inputs
        pivot_value = main_entry - sub_entry * prior_ratio
        ratio_next = sup_entry / pivot_value
        value_next = (unit_row[None, None, None, :] - sub_entry[..., None] * prior_value) / pivot_value[..., None]
        return ((ratio_next, value_next), (ratio_next, value_next))
    initial = (jnp.zeros((NSUB, FIELDS, L), jnp.float32), jnp.zeros((NSUB, FIELDS, L, P_SIZE), jnp.float32))
    _, (ratios, values) = lax.scan(forward, initial, bands)

    def backward(later_value, inputs):
        ratio_here, value_here = inputs
        current = value_here - ratio_here[..., None] * later_value
        return (current, current)
    _, solved = lax.scan(backward, jnp.zeros((NSUB, FIELDS, L, P_SIZE), jnp.float32), (ratios, values), reverse=True)
    position = jnp.arange(P_SIZE)
    interior = ((position > 0) & (position < P_SIZE - 1)).astype(jnp.float32)
    noise = jax.random.truncated_normal(jax.random.fold_in(key, 14), -3.0, 3.0, (NSUB, FIELDS, P_SIZE, P_SIZE, L), jnp.float32)
    inner_mask = (interior[:, None] * interior[None, :])[None, None, :, :, None]
    mixing = jnp.eye(P_SIZE, dtype=jnp.float32)[None, None, :, :, None] + 0.5 * noise / math.sqrt(P_SIZE - 2) * inner_mask
    return jnp.einsum('isflk,sfkjl->sfijl', solved, mixing, precision=lax.Precision.HIGHEST)


def block_levels(rng, dims, split, smallest, largest):
    def one(dim, blocks):
        draws = jax.random.uniform(jax.random.fold_in(jax.random.fold_in(rng, 6), dim), (blocks,), jnp.float32, smallest / len(split), largest / len(split))
        return jnp.repeat(jnp.exp(draws), dims[dim] // blocks).reshape((-1,) + (1,) * (len(dims) - dim - 1))

    loudness = one(*split[0])
    for cut in split[1:]:
        loudness = loudness * one(*cut)
    return loudness


def scatter_about(key, shape, scale, most, split=(), held_as=jnp.bfloat16):
    drawn = scale * jax.random.normal(key, shape, jnp.float32)
    if split:
        drawn = drawn * block_levels(key, shape, split, -0.22, 0.18)
    return jnp.clip(drawn, -most, most).astype(held_as)


def setup_inputs(seed: int = 0) -> dict:
    arg_keys = jax.random.split(jax.random.key(seed), 5)
    forcing = scatter_about(arg_keys[0], (FIELDS, NR, 2, MTOT, L), 4.0, 24.0, ((1, 8), (3, 16)), jnp.float32)
    slot_wavenumber = draw_slot_wavenumber(jax.random.fold_in(arg_keys[4], 71), 0)
    inverse = draw_inverse(jax.random.fold_in(arg_keys[4], 71), 0)
    edge_weights = draw_edge_weights(jax.random.fold_in(arg_keys[4], 71), 0)
    return {"forcing": forcing, "slot_wavenumber": slot_wavenumber, "inverse": inverse, "edge_weights": edge_weights}


HIGH = lax.Precision.HIGHEST


def local_solve(pair):
    block_inverse, block_source = pair
    return jnp.einsum('fpql,fqcml->fpcml', block_inverse, block_source, precision=HIGH)


def reference(forcing, slot_wavenumber, inverse, edge_weights):
    degree = jnp.arange(L, dtype=jnp.int32)
    kept_modes = (degree[None, :] >= slot_wavenumber[:, None]).astype(jnp.float32)
    position = jnp.arange(P_SIZE, dtype=jnp.int32)
    interior = ((position > 0) & (position < P_SIZE - 1)).astype(jnp.float32)
    source = forcing.reshape(FIELDS, NSUB, P_SIZE, 2, MTOT, L)
    source = source * kept_modes[None, None, None, None, :, :] * interior[None, None, :, None, None, None]
    source = jnp.transpose(source, (1, 0, 2, 3, 4, 5))
    particular = lax.map(local_solve, (inverse, source))
    low_row = edge_weights[:, 0, :]
    top_row = edge_weights[:, 1, :]
    low_slope = jnp.einsum('sp,sfpcml->sfcml', low_row, particular, precision=HIGH)
    top_slope = jnp.einsum('sp,sfpcml->sfcml', top_row, particular, precision=HIGH)
    lower_unit = inverse[:, :, :, 0, :]
    upper_unit = inverse[:, :, :, P_SIZE - 1, :]
    low_lower = jnp.einsum('sp,sfpl->sfl', low_row, lower_unit, precision=HIGH)
    low_upper = jnp.einsum('sp,sfpl->sfl', low_row, upper_unit, precision=HIGH)
    top_lower = jnp.einsum('sp,sfpl->sfl', top_row, lower_unit, precision=HIGH)
    top_upper = jnp.einsum('sp,sfpl->sfl', top_row, upper_unit, precision=HIGH)
    ratio_now = jnp.zeros((FIELDS, L), jnp.float32)
    reduced = jnp.zeros((FIELDS, 2, MTOT, L), jnp.float32)
    ratio_list = []
    reduced_list = []
    for level in range(NSUB - 1):
        lower_coef = top_lower[level]
        middle_coef = top_upper[level] - low_lower[level + 1]
        upper_coef = -low_upper[level + 1]
        right_side = low_slope[level + 1] - top_slope[level]
        pivot_value = middle_coef - lower_coef * ratio_now
        ratio_now = upper_coef / pivot_value
        reduced = (right_side - lower_coef[:, None, None, :] * reduced) / pivot_value[:, None, None, :]
        ratio_list.append(ratio_now)
        reduced_list.append(reduced)
    later_value = jnp.zeros((FIELDS, 2, MTOT, L), jnp.float32)
    interface = [later_value] * (NSUB - 1)
    for level in range(NSUB - 2, -1, -1):
        later_value = reduced_list[level] - ratio_list[level][:, None, None, :] * later_value
        interface[level] = later_value
    boundary = jnp.zeros((FIELDS, 2, MTOT, L), jnp.float32)
    lower_value = jnp.stack([boundary] + interface)
    upper_value = jnp.stack(interface + [boundary])
    solution = particular + lower_value[:, :, None] * lower_unit[:, :, :, None, None, :]
    solution = solution + upper_value[:, :, None] * upper_unit[:, :, :, None, None, :]
    return jnp.transpose(solution, (1, 0, 2, 3, 4, 5)).reshape(FIELDS, NR, 2, MTOT, L)
```

```python
import functools

import jax
import jax.numpy as jnp
from jax import lax
from jax.experimental import pallas as pl
from jax.experimental.pallas import tpu as pltpu
from jax.sharding import PartitionSpec as P

MESH = pl.DeviceIdType.MESH
F32 = jnp.float32
NP = 64
NS = 8
NM = 16
TILES = (2, 1, 3, 0)
STEPS = tuple((f, t) for f in range(2) for t in TILES)
NSTEP = len(STEPS)
PB = 8
QB = 16


def has_odd(k):
    return STEPS[k][1] >= 2


def odd_index(k):
    return STEPS[k][0] * 2 + STEPS[k][1] - 2


def iota(dim):
    return lax.broadcasted_iota(jnp.int32, (8, 128), dim)


def row(ref, *at):
    return jnp.broadcast_to(ref[at], (8, 128))


def flip_lanes(x):
    return jnp.take_along_axis(x, 127 - iota(1), axis=1)


def solve_kernel(
    forcing, slots, edges, inverse, packed, extras, modes,
    inv, raw, even, odd, even_part, odd_part, odd_flip, sent, weights, slopes, values, lasts, last_rows, own_modes,
    inv_sem, raw_sem, slope_send, slope_recv, field_send, field_recv, last_send, last_recv, mode_send, mode_recv,
):
    sub = lax.axis_index("sub")
    me = lax.axis_index("ma")
    y, x = me // 4, lax.rem(me, 4)
    subs = [lax.rem(sub + d, NS) for d in range(1, NS)]
    peers = []
    for dy in (2, 1, 3, 0):
        for dx in (2, 1, 3, 0):
            if dy or dx:
                peers.append(lax.rem(y + dy, 4) * 4 + lax.rem(x + dx, 4))

    barrier = pltpu.get_barrier_semaphore()
    for other in subs:
        pl.semaphore_signal(barrier, inc=1, device_id={"sub": other}, device_id_type=MESH)
    for other in peers:
        pl.semaphore_signal(barrier, inc=1, device_id={"ma": other}, device_id_type=MESH)

    def load(k):
        f, t = STEPS[k]
        lanes = pl.ds(t * 128, 128)
        return (
            pltpu.make_async_copy(inverse.at[f, :, :, lanes], inv.at[k], inv_sem.at[k]),
            pltpu.make_async_copy(forcing.at[f, :, :, lanes], raw.at[k], raw_sem.at[k]),
        )

    def start_load(k):
        for copy in load(k):
            copy.start()

    for k in range(3):
        start_load(k)

    pair = lax.rem(iota(0), 4)
    even_mode = jnp.zeros((8, 128), jnp.int32)
    odd_mode = jnp.zeros((8, 128), jnp.int32)
    for j in range(4):
        even_mode = jnp.where(pair == j, slots[2 * j], even_mode)
        odd_mode = jnp.where(pair == j, slots[2 * j + 1], odd_mode)
    own_modes[...] = even_mode.astype(F32)
    lane = iota(1)

    def slope_step(k):
        f, t = STEPS[k]
        for copy in load(k):
            copy.wait()
        if k + 3 < NSTEP:
            start_load(k + 3)
        even_kept = lane + t * 128 >= even_mode
        odd_kept = lane + t * 128 >= odd_mode
        zero = jnp.zeros((8, 128), F32)
        o = odd_index(k)

        def prepare(b, _):
            for i in range(8):
                q = b * 8 + i
                even[k, q] = jnp.where(even_kept, raw[k, q, pl.ds(0, 8, stride=2), :], zero)
                if has_odd(k):
                    odd[o, q] = jnp.where(odd_kept, raw[k, q, pl.ds(1, 8, stride=2), :], zero)
            return 0

        lax.fori_loop(0, NP // 8, prepare, 0)
        for q in (0, NP - 1):
            even[k, q] = zero
            if has_odd(k):
                odd[o, q] = zero

        def weigh(b, _):
            rows = pl.ds(pl.multiple_of(b * 8, 8), 8)
            low = [zero] * 2
            top = [zero] * 2
            for p in range(NP):
                block = inv[k, p, rows, :]
                low[p % 2] = low[p % 2] + edges[0, 0, p] * block
                top[p % 2] = top[p % 2] + edges[0, 1, p] * block
            weights[0, rows, :] = low[0] + low[1]
            weights[1, rows, :] = top[0] + top[1]
            return 0

        lax.fori_loop(0, NP // 8, weigh, 0)

        def gather(b, sums):
            sums = list(sums)
            for i in range(8):
                q = b * 8 + i
                for e in range(2):
                    weight = row(weights, e, pl.ds(q, 1), slice(None))
                    sums[e] = sums[e] + weight * even[k, q]
                    if has_odd(k):
                        sums[2 + e] = sums[2 + e] + weight * odd[o, q]
            return tuple(sums)

        sums = lax.fori_loop(0, NP // 8, gather, (zero,) * (4 if has_odd(k) else 2))
        for e in range(2):
            slopes[k, sub, e] = sums[e]
            for i, q in enumerate((0, NP - 1)):
                slopes[k, sub, 2, 2 * e + i : 2 * e + i + 1, :] = weights[e, q : q + 1, :]
            if has_odd(k):
                slopes[k, sub, 3 + e] = sums[2 + e]

    def slope_copies(k):
        count = 5 if has_odd(k) else 3
        here = slopes.at[k, sub, pl.ds(0, count)]
        return [
            pltpu.make_async_remote_copy(
                here, here, slope_send.at[k, i], slope_recv.at[k, i],
                device_id={"sub": other}, device_id_type=MESH,
            )
            for i, other in enumerate(subs)
        ]

    def particular_step(k):
        o = odd_index(k)
        both = has_odd(k)
        zero = jnp.zeros((8, 128), F32)

        def block(b, _):
            def inner(c, sums):
                sums = list(sums)
                for i in range(QB):
                    q = c * QB + i
                    source = even[k, q]
                    other = odd[o, q] if both else None
                    for j in range(PB):
                        weight = row(inv, k, b * PB + j, pl.ds(q, 1), slice(None))
                        sums[j] = sums[j] + weight * source
                        if both:
                            sums[PB + j] = sums[PB + j] + weight * other
                return tuple(sums)

            sums = lax.fori_loop(0, NP // QB, inner, (zero,) * (2 * PB if both else PB))
            for j in range(PB):
                even_part[k, b * PB + j] = sums[j]
                if both:
                    odd_part[o, b * PB + j] = sums[PB + j]
            return 0

        lax.fori_loop(0, NP // PB, block, 0)

    def interface(k, low_at, top_at, which):
        ratio = jnp.zeros((8, 128), F32)
        reduced = jnp.zeros((8, 128), F32)
        ratios, reduceds = [], []
        for s in range(NS - 1):
            lower = row(slopes, k, s, 2, slice(2, 3), slice(None))
            middle = row(slopes, k, s, 2, slice(3, 4), slice(None)) - row(slopes, k, s + 1, 2, slice(0, 1), slice(None))
            upper = -row(slopes, k, s + 1, 2, slice(1, 2), slice(None))
            right = slopes[k, s + 1, low_at] - slopes[k, s, top_at]
            pivot = middle - lower * ratio
            ratio = upper / pivot
            reduced = (right - lower * reduced) / pivot
            ratios.append(ratio)
            reduceds.append(reduced)
        later = jnp.zeros((8, 128), F32)
        values[which, 0] = later
        values[which, NS] = later
        for s in range(NS - 2, -1, -1):
            later = reduceds[s] - ratios[s] * later
            values[which, s + 1] = later
        return values[which, sub], values[which, sub + 1]

    def finish_step(k):
        f, t = STEPS[k]
        o = odd_index(k)
        for copy in slope_copies(k):
            copy.wait()
        below, above = interface(k, 0, 1, 0)
        if has_odd(k):
            odd_below, odd_above = interface(k, 3, 4, 1)
        position = lane + t * 128
        even_kept = position >= even_mode
        meets = position == even_mode
        merged = f * 2 + 1 - t

        def block(b, _):
            last = jnp.zeros((8, 128), F32)
            for i in range(4):
                p = b * 4 + i
                first = row(inv, k, p, slice(0, 1), slice(None))
                final = row(inv, k, p, slice(NP - 1, NP), slice(None))
                field = even_part[k, p] + below * first
                field = field + above * final
                if has_odd(k):
                    other = odd_part[o, p] + odd_below * first
                    other = other + odd_above * final
                    odd_flip[o, p] = flip_lanes(other)
                else:
                    other = odd_flip[merged, p]
                    at = f * 32 + i * 8
                    value = jnp.sum(jnp.where(meets, other, 0.0), axis=1, keepdims=True)
                    last = last + jnp.where(lane == iota(0) + at, value, 0.0)
                    field = jnp.where(even_kept, field, other)
                sent[k, p] = field
            if not has_odd(k):
                if k == 1:
                    lasts[b] = last
                else:
                    lasts[b] = lasts[b] + last
            return 0

        lax.fori_loop(0, NM, block, 0)
        packed[k, me] = sent[k, pl.ds(me * 4, 4)]

    def field_copies(k):
        return [
            pltpu.make_async_remote_copy(
                sent.at[k, pl.ds(other * 4, 4)], packed.at[k, me], field_send.at[k, i], field_recv.at[k, i],
                device_id={"ma": other}, device_id_type=MESH,
            )
            for i, other in enumerate(peers)
        ]

    def mode_copies():
        return [
            pltpu.make_async_remote_copy(
                own_modes, modes.at[me], mode_send.at[i], mode_recv.at[i],
                device_id={"ma": other}, device_id_type=MESH,
            )
            for i, other in enumerate(peers)
        ]

    def last_copies():
        return [
            pltpu.make_async_remote_copy(
                last_rows.at[other], extras.at[me], last_send.at[i], last_recv.at[i],
                device_id={"ma": other}, device_id_type=MESH,
            )
            for i, other in enumerate(peers)
        ]

    def start(copies):
        for copy in copies:
            copy.start()

    slope_step(0)
    pl.semaphore_wait(barrier, len(subs) + len(peers))
    start(slope_copies(0))
    start(mode_copies())
    particular_step(0)
    slope_step(1)
    start(slope_copies(1))
    particular_step(1)
    slope_step(2)
    start(slope_copies(2))
    for k in range(NSTEP):
        finish_step(k)
        start(field_copies(k))
        if k + 2 < NSTEP:
            particular_step(k + 2)
        if k + 3 < NSTEP:
            slope_step(k + 3)
            start(slope_copies(k + 3))

    for a in range(NM):
        last_rows[a] = jnp.sum(lasts[a], axis=0, keepdims=True)
    start(last_copies())
    extras[me] = last_rows[me]
    modes[me] = own_modes[...]
    for copies in [mode_copies()] + [field_copies(k) for k in range(NSTEP)] + [last_copies()]:
        for copy in copies:
            copy.wait()


def unpack_kernel(packed, extras, modes, out):
    step = pl.program_id(0)
    f = step // 4
    p = lax.rem(step, 4)
    lane = iota(1)
    sublane = iota(0)
    is_odd = lax.rem(sublane, 2) == 1
    at = {t: TILES.index(t) for t in TILES}
    pick = [sublane // 2, sublane // 2 + 4]

    def spread(value, c):
        return jnp.take_along_axis(value, pick[c], axis=0)

    def block(a, _):
        mode = modes[a].astype(jnp.int32)
        chosen = jnp.where(lane == f * 32 + p * 8 + sublane, jnp.broadcast_to(extras[a], (8, 128)), 0.0)
        extra = jnp.broadcast_to(jnp.sum(chosen, axis=1, keepdims=True), (8, 128))
        for t in range(4):
            value = packed[f * 4 + at[t], a, p]
            rows = pl.ds(pl.multiple_of(a * 8, 8), 8)
            if t < 2:
                even = jnp.where(lane + t * 128 >= mode, value, 0.0)
                other = None
            else:
                even = value
                merged = packed[f * 4 + at[3 - t], a, p]
                position = lane + (3 - t) * 128
                other = jnp.where(position < mode, merged, jnp.where(position == mode, extra, 0.0))
                other = flip_lanes(other)
            for c in range(2):
                tile = jnp.where(is_odd, 0.0 if other is None else spread(other, c), spread(even, c))
                out[0, 0, c, rows, t * 128 : t * 128 + 128] = tile
        return 0

    lax.fori_loop(0, NM, block, 0)


def body(forcing, slot_wavenumber, inverse, edge_weights):
    vmem = pl.BlockSpec(memory_space=pltpu.VMEM)
    smem = pl.BlockSpec(memory_space=pltpu.SMEM)
    anywhere = pl.BlockSpec(memory_space=pl.ANY)
    dma = pltpu.SemaphoreType.DMA
    packed, extras, modes = pl.pallas_call(
        solve_kernel,
        out_shape=(
            jax.ShapeDtypeStruct((NSTEP, NM, 4, 8, 128), F32),
            jax.ShapeDtypeStruct((NM, 1, 128), F32),
            jax.ShapeDtypeStruct((NM, 8, 128), F32),
        ),
        in_specs=[anywhere, smem, smem, anywhere],
        out_specs=(vmem, vmem, vmem),
        scratch_shapes=[
            pltpu.VMEM((NSTEP, NP, NP, 128), F32),
            pltpu.VMEM((NSTEP, NP, 16, 128), F32),
            pltpu.VMEM((NSTEP, NP, 8, 128), F32),
            pltpu.VMEM((4, NP, 8, 128), F32),
            pltpu.VMEM((NSTEP, NP, 8, 128), F32),
            pltpu.VMEM((4, NP, 8, 128), F32),
            pltpu.VMEM((4, NP, 8, 128), F32),
            pltpu.VMEM((NSTEP, NP, 8, 128), F32),
            pltpu.VMEM((2, NP, 128), F32),
            pltpu.VMEM((NSTEP, NS, 5, 8, 128), F32),
            pltpu.VMEM((2, NS + 1, 8, 128), F32),
            pltpu.VMEM((NM, 8, 128), F32),
            pltpu.VMEM((NM, 1, 128), F32),
            pltpu.VMEM((8, 128), F32),
            dma((NSTEP,)),
            dma((NSTEP,)),
            dma((NSTEP, NS - 1)),
            dma((NSTEP, NS - 1)),
            dma((NSTEP, NM - 1)),
            dma((NSTEP, NM - 1)),
            dma((NM - 1,)),
            dma((NM - 1,)),
            dma((NM - 1,)),
            dma((NM - 1,)),
        ],
        compiler_params=pltpu.CompilerParams(
            collective_id=0, has_side_effects=True, vmem_limit_bytes=48 * 1024 * 1024
        ),
        name="solve_and_exchange",
    )(forcing.reshape(2, NP, 16, 512), slot_wavenumber, edge_weights, inverse[0])
    return pl.pallas_call(
        unpack_kernel,
        out_shape=jax.ShapeDtypeStruct((2, 4, 2, 128, 512), F32),
        grid=(8,),
        in_specs=[vmem, vmem, vmem],
        out_specs=pl.BlockSpec((1, 1, 2, 128, 512), lambda i: (i // 4, lax.rem(i, 4), 0, 0, 0)),
        compiler_params=pltpu.CompilerParams(vmem_limit_bytes=16 * 1024 * 1024),
        name="unpack",
    )(packed, extras, modes)


def solution(mesh):
    return jax.shard_map(
        body,
        mesh=mesh,
        in_specs=(
            P(None, "sub", None, "ma", None),
            P("ma"),
            P("sub", None, None, None, None),
            P("sub", None, None),
        ),
        out_specs=P(None, ("sub", "ma"), None, None, None),
        check_vma=False,
    )
```

```python
import jax
import jax.numpy as jnp
from jax import lax
from jax.experimental import pallas as pl
from jax.experimental.pallas import tpu as pltpu
from jax.sharding import PartitionSpec as P

MESH = pl.DeviceIdType.MESH
F32 = jnp.float32
NP = 64
NS = 8
NM = 16
TILES = (2, 1, 3, 0)
STEPS = tuple((f, t) for f in range(2) for t in TILES)
NSTEP = len(STEPS)
AHEAD = 3
PB = 8
QB = 31
FB = 32
ORDER = "S0 S1 P0 S2 F0 P1 F1 S3 S4 P2 F2 S5 S6 P3 F3 S7 P4 F4 P5 F5 P6 F6 P7 F7"


def has_odd(k):
    return STEPS[k][1] >= 2


def half(k):
    return k // 2


def iota(dim):
    return lax.broadcasted_iota(jnp.int32, (8, 128), dim)


def row(ref, *at):
    return jnp.broadcast_to(ref[at], (8, 128))


def flip_lanes(x):
    return jnp.take_along_axis(x, 127 - iota(1), axis=1)


def solve_kernel(
    forcing, slot_hbm, edge_hbm, inverse, out,
    slots, edges, inv, raw, even, odd, even_part, odd_part, odd_flip, sent, packed, weights, splats,
    even_slopes, odd_slopes, factors, values, last_rows, extras, own_modes, modes,
    small_sem, inv_sem, raw_sem, even_send, even_recv, odd_send, odd_recv,
    field_send, field_recv, last_send, last_recv, mode_send, mode_recv,
):
    sub = lax.axis_index("sub")
    me = lax.axis_index("ma")
    y, x = me // 4, lax.rem(me, 4)
    subs = [lax.rem(sub + d, NS) for d in range(1, NS)]
    peers = []
    for dy in (2, 1, 3, 0):
        for dx in (2, 1, 3, 0):
            if dy or dx:
                peers.append(lax.rem(y + dy, 4) * 4 + lax.rem(x + dx, 4))

    def load(k):
        f, t = STEPS[k]
        lanes = pl.ds(t * 128, 128)
        return (
            pltpu.make_async_copy(inverse.at[f, :, :, lanes], inv.at[k], inv_sem.at[k]),
            pltpu.make_async_copy(forcing.at[f, :, :, lanes], raw.at[k], raw_sem.at[k]),
        )

    def start(copies):
        for copy in copies:
            copy.start()

    start(load(0))
    small = (
        pltpu.make_async_copy(slot_hbm, slots, small_sem.at[0]),
        pltpu.make_async_copy(edge_hbm, edges, small_sem.at[1]),
    )
    start(small)
    barrier = pltpu.get_barrier_semaphore()
    for other in subs:
        pl.semaphore_signal(barrier, inc=1, device_id={"sub": other}, device_id_type=MESH)
    for other in peers:
        pl.semaphore_signal(barrier, inc=1, device_id={"ma": other}, device_id_type=MESH)
    for k in range(1, AHEAD):
        start(load(k))

    for copy in small:
        copy.wait()
    zero = jnp.zeros((8, 128), F32)
    lane = iota(1)
    sublane = iota(0)
    pair = lax.rem(sublane, 4)
    even_mode = jnp.zeros((8, 128), jnp.int32)
    odd_mode = jnp.zeros((8, 128), jnp.int32)
    for j in range(4):
        even_mode = jnp.where(pair == j, slots[2 * j], even_mode)
        odd_mode = jnp.where(pair == j, slots[2 * j + 1], odd_mode)
    own_modes[...] = even_mode.astype(F32)
    for e in range(2):
        for p in range(NP):
            splats[e, p] = jnp.full((8, 128), edges[0, e, p], F32)

    def prepare(k, which):
        f, t = STEPS[k]
        kept = lane + t * 128 >= (even_mode if which == 0 else odd_mode)
        target = even.at[k] if which == 0 else odd.at[half(k)]

        def block(b, _):
            for i in range(8):
                q = b * 8 + i
                target[q] = jnp.where(kept, raw[k, q, pl.ds(which, 8, stride=2), :], zero)
            return 0

        lax.fori_loop(0, NP // 8, block, 0)
        target[0] = zero
        target[NP - 1] = zero

    def weigh(k):
        def block(b, _):
            def inner(c, sums):
                sums = list(sums)
                for j in range(16):
                    p = c * 16 + j
                    low, top = splats[0, p], splats[1, p]
                    for i in range(4):
                        tile = inv[k, p, pl.ds(pl.multiple_of(b * 32 + i * 8, 8), 8), :]
                        sums[i] = sums[i] + low * tile
                        sums[4 + i] = sums[4 + i] + top * tile
                return tuple(sums)

            sums = lax.fori_loop(0, NP // 16, inner, (zero,) * 8)
            for i in range(4):
                rows = pl.ds(pl.multiple_of(b * 32 + i * 8, 8), 8)
                weights[0, rows, :] = sums[i]
                weights[1, rows, :] = sums[4 + i]
            return 0

        lax.fori_loop(0, NP // 32, block, 0)

    def slope_sums(k, which):
        source = even.at[k] if which == 0 else odd.at[half(k)]
        def block(b, sums):
            sums = list(sums)
            for i in range(8):
                q = b * 8 + i
                for e in range(2):
                    at = 2 * e + i % 2
                    sums[at] = sums[at] + row(weights, e, pl.ds(q, 1), slice(None)) * source[q]
            return tuple(sums)

        sums = lax.fori_loop(0, NP // 8, block, (zero,) * 4)
        return sums[0] + sums[1], sums[2] + sums[3]

    def even_copies(k):
        here = even_slopes.at[k, sub]
        return [
            pltpu.make_async_remote_copy(
                here, here, even_send.at[k], even_recv.at[k], device_id={"sub": other}, device_id_type=MESH
            )
            for other in subs
        ]

    def odd_copies(k):
        here = odd_slopes.at[half(k), sub]
        return [
            pltpu.make_async_remote_copy(
                here, here, odd_send.at[half(k)], odd_recv.at[half(k)], device_id={"sub": other}, device_id_type=MESH
            )
            for other in subs
        ]

    def even_all(k):
        most = even_slopes.at[k, pl.ds(0, NS - 1)]
        return pltpu.make_async_remote_copy(
            most, most, even_send.at[k], even_recv.at[k], device_id={"sub": subs[0]}, device_id_type=MESH
        )

    def odd_all(k):
        most = odd_slopes.at[half(k), pl.ds(0, NS - 1)]
        return pltpu.make_async_remote_copy(
            most, most, odd_send.at[half(k)], odd_recv.at[half(k)], device_id={"sub": subs[0]}, device_id_type=MESH
        )

    def slope_step(k, before_send=None):
        for copy in load(k):
            copy.wait()
        if k + AHEAD < NSTEP:
            start(load(k + AHEAD))
        prepare(k, 0)
        weigh(k)
        low, top = slope_sums(k, 0)
        even_slopes[k, sub, 0] = low
        even_slopes[k, sub, 1] = top
        for e in range(2):
            for i, q in enumerate((0, NP - 1)):
                even_slopes[k, sub, 2, 2 * e + i : 2 * e + i + 1, :] = weights[e, q : q + 1, :]
        if before_send is not None:
            before_send()
        start(even_copies(k))
        if has_odd(k):
            prepare(k, 1)
            low, top = slope_sums(k, 1)
            odd_slopes[half(k), sub, 0] = low
            odd_slopes[half(k), sub, 1] = top
            start(odd_copies(k))

    def ends(k, p):
        return (
            row(inv, k, p, slice(0, 1), slice(None)),
            row(inv, k, p, slice(NP - 1, NP), slice(None)),
        )

    def particular_step(k):
        both = has_odd(k)
        o = half(k)

        def block(b, _):
            def inner(c, sums):
                sums = list(sums)
                for i in range(QB):
                    q = 1 + c * QB + i
                    source = even[k, q]
                    other = odd[o, q] if both else None
                    for j in range(PB):
                        weight = row(inv, k, b * PB + j, pl.ds(q, 1), slice(None))
                        sums[j] = sums[j] + weight * source
                        if both:
                            sums[PB + j] = sums[PB + j] + weight * other
                return tuple(sums)

            sums = lax.fori_loop(0, (NP - 2) // QB, inner, (zero,) * (2 * PB if both else PB))
            for j in range(PB):
                p = b * PB + j
                even_part[k, p] = sums[j]
                if both:
                    odd_part[o, p] = sums[PB + j]
            return 0

        lax.fori_loop(0, NP // PB, block, 0)

    def factor(k):
        def influence(s, i):
            return row(even_slopes, k, s, 2, slice(i, i + 1), slice(None))

        last = NS - 2
        lower = [influence(s, 2) for s in range(NS - 1)]
        middle = [influence(s, 3) - influence(s + 1, 0) for s in range(NS - 1)]
        upper = [-influence(s + 1, 1) for s in range(NS - 1)]
        ratio = [zero] * (NS - 1)
        scale = [zero] * (NS - 1)
        for s in range(3):
            scale[s] = 1.0 / (middle[s] - lower[s] * ratio[s - 1] if s else middle[s])
            ratio[s] = upper[s] * scale[s]
            r = last - s
            scale[r] = 1.0 / (middle[r] - upper[r] * ratio[r + 1] if s else middle[r])
            ratio[r] = lower[r] * scale[r]
        scale[3] = 1.0 / ((middle[3] - lower[3] * ratio[2]) - upper[3] * ratio[4])
        for s in range(NS - 1):
            factors[0, s] = lower[s]
            factors[1, s] = upper[s]
            factors[2, s] = ratio[s]
            factors[3, s] = scale[s]

    def interface(k, which):
        slopes = even_slopes.at[k] if which == 0 else odd_slopes.at[half(k)]
        last = NS - 2
        right = [slopes[s + 1, 0] - slopes[s, 1] for s in range(NS - 1)]
        lower = [factors[0, s] for s in range(NS - 1)]
        upper = [factors[1, s] for s in range(NS - 1)]
        ratio = [factors[2, s] for s in range(NS - 1)]
        scale = [factors[3, s] for s in range(NS - 1)]
        reduced = [zero] * (NS - 1)
        for s in range(3):
            r = last - s
            reduced[s] = (right[s] - lower[s] * reduced[s - 1] if s else right[s]) * scale[s]
            reduced[r] = (right[r] - upper[r] * reduced[r + 1] if s else right[r]) * scale[r]
        found = [zero] * (NS - 1)
        found[3] = ((right[3] - lower[3] * reduced[2]) - upper[3] * reduced[4]) * scale[3]
        for s in (2, 1, 0):
            found[s] = reduced[s] - ratio[s] * found[s + 1]
            found[last - s] = reduced[last - s] - ratio[last - s] * found[last - s - 1]
        values[which, 0] = zero
        values[which, NS] = zero
        for s in range(NS - 1):
            values[which, s + 1] = found[s]
        return values[which, sub], values[which, sub + 1]

    def finish_step(k):
        f, t = STEPS[k]
        u = half(k)
        even_all(k).wait()
        factor(k)
        below, above = interface(k, 0)
        position = lane + t * 128
        even_kept = position >= even_mode

        def block(b, _):
            for i in range(FB):
                p = b * FB + i
                first, final = ends(k, p)
                field = (even_part[k, p] + below * first) + above * final
                if not has_odd(k):
                    field = jnp.where(even_kept, field, odd_flip[u, p])
                sent[k, p] = field
            return 0

        lax.fori_loop(0, NP // FB, block, 0)
        packed[k, me] = sent[k, pl.ds(me * 4, 4)]
        start(field_copies(k))
        if has_odd(k):
            odd_all(k).wait()
            odd_below, odd_above = interface(k, 1)
            meets = lane + (3 - t) * 128 == even_mode

            def odd_block(b, _):
                for a in range(FB // 4):
                    last = zero
                    for i in range(4):
                        p = b * FB + a * 4 + i
                        first, final = ends(k, p)
                        other = flip_lanes((odd_part[u, p] + odd_below * first) + odd_above * final)
                        odd_flip[u, p] = other
                        value = jnp.sum(jnp.where(meets, other, 0.0), axis=1, keepdims=True)
                        last = jnp.where(lane == sublane + i * 8, value, last)
                    last_rows[u, b * (FB // 4) + a] = jnp.sum(last, axis=0, keepdims=True)
                return 0

            lax.fori_loop(0, NP // FB, odd_block, 0)
            extras[u, me] = last_rows[u, me]
            start(last_copies(u))

    def field_copies(k):
        return [
            pltpu.make_async_remote_copy(
                sent.at[k, pl.ds(other * 4, 4)], packed.at[k, me], field_send.at[k], field_recv.at[k],
                device_id={"ma": other}, device_id_type=MESH,
            )
            for other in peers
        ]

    def field_all(k):
        return pltpu.make_async_remote_copy(
            sent.at[k, pl.ds(0, NP - 4)], packed.at[k, pl.ds(0, NM - 1)], field_send.at[k], field_recv.at[k],
            device_id={"ma": peers[0]}, device_id_type=MESH,
        )

    def last_copies(u):
        return [
            pltpu.make_async_remote_copy(
                last_rows.at[u, other], extras.at[u, me], last_send.at[u], last_recv.at[u],
                device_id={"ma": other}, device_id_type=MESH,
            )
            for other in peers
        ]

    def last_all(u):
        return pltpu.make_async_remote_copy(
            last_rows.at[u, pl.ds(0, NM - 1)], extras.at[u, pl.ds(0, NM - 1)], last_send.at[u], last_recv.at[u],
            device_id={"ma": peers[0]}, device_id_type=MESH,
        )

    def mode_copies():
        return [
            pltpu.make_async_remote_copy(
                own_modes, modes.at[me], mode_send, mode_recv, device_id={"ma": other}, device_id_type=MESH
            )
            for other in peers
        ]

    def mode_all():
        most = modes.at[pl.ds(0, NM - 1)]
        return pltpu.make_async_remote_copy(
            most, most, mode_send, mode_recv, device_id={"ma": peers[0]}, device_id_type=MESH
        )

    def unpack(u):
        f, t = STEPS[2 * u]
        near = 3 - t
        is_odd = lax.rem(sublane, 2) == 1
        pick = [sublane // 2, sublane // 2 + 4]

        def spread(value, c):
            return jnp.take_along_axis(value, pick[c], axis=0)

        def block(b, _):
            for i in range(4):
                a = b * 4 + i
                mode = modes[a].astype(jnp.int32)
                even_kept = lane + near * 128 >= mode
                odd_at = lane + t * 128 + mode
                rows = pl.ds(pl.multiple_of(a * 8, 8), 8)
                row_extras = row(extras, u, a)
                for p in range(4):
                    merged = packed[2 * u + 1, a, p]
                    extra = jnp.take_along_axis(row_extras, sublane + p * 8, axis=1)
                    other = jnp.where(odd_at > 511, flip_lanes(merged), jnp.where(odd_at == 511, extra, 0.0))
                    far = packed[2 * u, a, p]
                    close = jnp.where(even_kept, merged, 0.0)
                    for c in range(2):
                        out[f, p, c, rows, t * 128 : t * 128 + 128] = jnp.where(
                            is_odd, spread(other, c), spread(far, c)
                        )
                        out[f, p, c, rows, near * 128 : near * 128 + 128] = jnp.where(is_odd, 0.0, spread(close, c))
            return 0

        lax.fori_loop(0, NM // 4, block, 0)

    def greet():
        pl.semaphore_wait(barrier, len(subs) + len(peers))
        modes[me] = own_modes[...]

    for item in ORDER.split():
        k = int(item[1])
        if item[0] == "S":
            slope_step(k, greet if k == 0 else None)
            if k == 0:
                start(mode_copies())
        elif item[0] == "P":
            particular_step(k)
        else:
            finish_step(k)

    mode_all().wait()
    for u in range(NSTEP // 2):
        field_all(2 * u).wait()
        field_all(2 * u + 1).wait()
        last_all(u).wait()
        unpack(u)


def body(forcing, slot_wavenumber, inverse, edge_weights):
    vmem = pl.BlockSpec(memory_space=pltpu.VMEM)
    anywhere = pl.BlockSpec(memory_space=pl.ANY)
    dma = pltpu.SemaphoreType.DMA
    units = NSTEP // 2
    return pl.pallas_call(
        solve_kernel,
        out_shape=jax.ShapeDtypeStruct((2, 4, 2, 128, 512), F32),
        in_specs=[anywhere] * 4,
        out_specs=vmem,
        scratch_shapes=[
            pltpu.SMEM((8,), jnp.int32),
            pltpu.SMEM((1, 2, NP), F32),
            pltpu.VMEM((NSTEP, NP, NP, 128), F32),
            pltpu.VMEM((NSTEP, NP, 16, 128), F32),
            pltpu.VMEM((NSTEP, NP, 8, 128), F32),
            pltpu.VMEM((units, NP, 8, 128), F32),
            pltpu.VMEM((NSTEP, NP, 8, 128), F32),
            pltpu.VMEM((units, NP, 8, 128), F32),
            pltpu.VMEM((units, NP, 8, 128), F32),
            pltpu.VMEM((NSTEP, NP, 8, 128), F32),
            pltpu.VMEM((NSTEP, NM, 4, 8, 128), F32),
            pltpu.VMEM((2, NP, 128), F32),
            pltpu.VMEM((2, NP, 8, 128), F32),
            pltpu.VMEM((NSTEP, NS, 3, 8, 128), F32),
            pltpu.VMEM((units, NS, 2, 8, 128), F32),
            pltpu.VMEM((4, NS - 1, 8, 128), F32),
            pltpu.VMEM((2, NS + 1, 8, 128), F32),
            pltpu.VMEM((units, NM, 1, 128), F32),
            pltpu.VMEM((units, NM, 1, 128), F32),
            pltpu.VMEM((8, 128), F32),
            pltpu.VMEM((NM, 8, 128), F32),
            dma((2,)),
            dma((NSTEP,)),
            dma((NSTEP,)),
            dma((NSTEP,)),
            dma((NSTEP,)),
            dma((units,)),
            dma((units,)),
            dma((NSTEP,)),
            dma((NSTEP,)),
            dma((units,)),
            dma((units,)),
            dma,
            dma,
        ],
        compiler_params=pltpu.CompilerParams(
            collective_id=0, has_side_effects=True, vmem_limit_bytes=48 * 1024 * 1024
        ),
        name="solve_and_exchange",
    )(forcing.reshape(2, NP, 16, 512), slot_wavenumber, edge_weights, inverse[0])


def solution(mesh):
    return jax.shard_map(
        body,
        mesh=mesh,
        in_specs=(
            P(None, "sub", None, "ma", None),
            P("ma"),
            P("sub", None, None, None, None),
            P("sub", None, None),
        ),
        out_specs=P(None, ("sub", "ma"), None, None, None),
        check_vma=False,
    )
```

```python
import jax
import jax.numpy as jnp
from jax import lax
from jax.experimental import pallas as pl
from jax.experimental.pallas import tpu as pltpu
from jax.sharding import PartitionSpec as P

MESH = pl.DeviceIdType.MESH
F32 = jnp.float32
NP = 64
NS = 8
NM = 16
TILES = (2, 1, 3, 0)
STEPS = tuple((f, t) for f in range(2) for t in TILES)
NSTEP = len(STEPS)
AHEAD = 3
PB = 8
QB = 31
FB = 32
ORDER = ("S0", "E0", "R0", "S1", "O0", "S2", "P1", "F0", "F1", "S3", "P2", "F2", "S4", "P3", "F3", "S5", "P4", "F4", "S6", "P5", "F5", "S7", "P6", "F6", "P7", "F7")


def has_odd(k):
    return STEPS[k][1] >= 2


def half(k):
    return k // 2


def iota(dim):
    return lax.broadcasted_iota(jnp.int32, (8, 128), dim)


def row(ref, *at):
    return jnp.broadcast_to(ref[at], (8, 128))


def flip_lanes(x):
    return jnp.take_along_axis(x, 127 - iota(1), axis=1)


def solve_kernel(
    forcing, slot_hbm, edge_hbm, inverse, out,
    slots, edges, inv, raw, even, odd, even_part, odd_part, odd_flip, sent, packed, weights, splats,
    even_slopes, odd_slopes, factors, values, last_rows, extras, own_modes, modes, own_ends, far_ends,
    small_sem, inv_sem, raw_sem, even_send, even_recv, odd_send, odd_recv,
    field_send, field_recv, last_send, last_recv, mode_send, mode_recv, end_send, end_recv,
):
    sub = lax.axis_index("sub")
    me = lax.axis_index("ma")
    y, x = me // 4, lax.rem(me, 4)
    chip, core = sub // 2, lax.rem(sub, 2)
    subs = []
    for dz in (2, 1, 3, 0):
        for dc in (0, 1):
            if dz or dc:
                subs.append(lax.rem(chip + dz, 4) * 2 + lax.rem(core + dc, 2))
    peers = []
    for dy in (2, 1, 3, 0):
        for dx in (2, 1, 3, 0):
            if dy or dx:
                peers.append(lax.rem(y + dy, 4) * 4 + lax.rem(x + dx, 4))

    def load(k):
        f, t = STEPS[k]
        lanes = pl.ds(t * 128, 128)
        return (
            pltpu.make_async_copy(forcing.at[f, :, :, lanes], raw.at[k], raw_sem.at[k]),
            pltpu.make_async_copy(inverse.at[f, :, :, lanes], inv.at[k], inv_sem.at[k]),
        )

    def start(copies):
        for copy in copies:
            copy.start()

    start(load(0))
    small = (
        pltpu.make_async_copy(slot_hbm, slots, small_sem.at[0]),
        pltpu.make_async_copy(edge_hbm, edges, small_sem.at[1]),
    )
    start(small)
    barrier = pltpu.get_barrier_semaphore()
    for other in subs:
        pl.semaphore_signal(barrier, inc=1, device_id={"sub": other}, device_id_type=MESH)
    for other in peers:
        pl.semaphore_signal(barrier, inc=1, device_id={"ma": other}, device_id_type=MESH)
    for k in range(1, AHEAD):
        start(load(k))

    for copy in small:
        copy.wait()
    zero = jnp.zeros((8, 128), F32)
    lane = iota(1)
    sublane = iota(0)
    pair = lax.rem(sublane, 4)
    even_mode = jnp.zeros((8, 128), jnp.int32)
    odd_mode = jnp.zeros((8, 128), jnp.int32)
    for j in range(4):
        even_mode = jnp.where(pair == j, slots[2 * j], even_mode)
        odd_mode = jnp.where(pair == j, slots[2 * j + 1], odd_mode)
    own_modes[...] = even_mode.astype(F32)
    for e in range(2):
        for p in range(NP):
            splats[e, p] = jnp.full((8, 128), edges[0, e, p], F32)

    def prepare(k, which):
        f, t = STEPS[k]
        kept = lane + t * 128 >= (even_mode if which == 0 else odd_mode)
        target = even.at[k] if which == 0 else odd.at[half(k)]

        def block(b, _):
            for i in range(8):
                q = b * 8 + i
                target[q] = jnp.where(kept, raw[k, q, pl.ds(which, 8, stride=2), :], zero)
            return 0

        lax.fori_loop(0, NP // 8, block, 0)
        target[0] = zero
        target[NP - 1] = zero

    def weigh(k):
        def block(b, _):
            def inner(c, sums):
                sums = list(sums)
                for j in range(16):
                    p = c * 16 + j
                    low, top = splats[0, p], splats[1, p]
                    for i in range(4):
                        tile = inv[k, p, pl.ds(pl.multiple_of(b * 32 + i * 8, 8), 8), :]
                        sums[i] = sums[i] + low * tile
                        sums[4 + i] = sums[4 + i] + top * tile
                return tuple(sums)

            sums = lax.fori_loop(0, NP // 16, inner, (zero,) * 8)
            for i in range(4):
                rows = pl.ds(pl.multiple_of(b * 32 + i * 8, 8), 8)
                weights[0, rows, :] = sums[i]
                weights[1, rows, :] = sums[4 + i]
            return 0

        lax.fori_loop(0, NP // 32, block, 0)

    def slope_sums(k, which):
        source = even.at[k] if which == 0 else odd.at[half(k)]
        def block(b, sums):
            sums = list(sums)
            for i in range(8):
                q = b * 8 + i
                for e in range(2):
                    at = 2 * e + i % 2
                    sums[at] = sums[at] + row(weights, e, pl.ds(q, 1), slice(None)) * source[q]
            return tuple(sums)

        sums = lax.fori_loop(0, NP // 8, block, (zero,) * 4)
        return sums[0] + sums[1], sums[2] + sums[3]

    def even_copies(k):
        here = even_slopes.at[k, sub]
        return [
            pltpu.make_async_remote_copy(
                here, here, even_send.at[k], even_recv.at[k], device_id={"sub": other}, device_id_type=MESH
            )
            for other in subs
        ]

    def odd_copies(k):
        here = odd_slopes.at[half(k), sub]
        return [
            pltpu.make_async_remote_copy(
                here, here, odd_send.at[half(k)], odd_recv.at[half(k)], device_id={"sub": other}, device_id_type=MESH
            )
            for other in subs
        ]

    def even_all(k):
        most = even_slopes.at[k, pl.ds(0, NS - 1)]
        return pltpu.make_async_remote_copy(
            most, most, even_send.at[k], even_recv.at[k], device_id={"sub": subs[0]}, device_id_type=MESH
        )

    def odd_all(k):
        most = odd_slopes.at[half(k), pl.ds(0, NS - 1)]
        return pltpu.make_async_remote_copy(
            most, most, odd_send.at[half(k)], odd_recv.at[half(k)], device_id={"sub": subs[0]}, device_id_type=MESH
        )

    def slope_step(k, before_send=None):
        source_copy, inverse_copy = load(k)
        source_copy.wait()
        prepare(k, 0)
        if has_odd(k):
            prepare(k, 1)
        inverse_copy.wait()
        if k + AHEAD < NSTEP:
            start(load(k + AHEAD))
        weigh(k)
        low, top = slope_sums(k, 0)
        even_slopes[k, sub, 0] = low
        even_slopes[k, sub, 1] = top
        for e in range(2):
            for i, q in enumerate((0, NP - 1)):
                even_slopes[k, sub, 2, 2 * e + i : 2 * e + i + 1, :] = weights[e, q : q + 1, :]
        if before_send is not None:
            before_send()
        start(even_copies(k))
        if has_odd(k):
            low, top = slope_sums(k, 1)
            odd_slopes[half(k), sub, 0] = low
            odd_slopes[half(k), sub, 1] = top
            start(odd_copies(k))

    def ends(k, p):
        return (
            row(inv, k, p, slice(0, 1), slice(None)),
            row(inv, k, p, slice(NP - 1, NP), slice(None)),
        )

    def particular_step(k, parts):
        o = half(k)

        def block(b, _):
            def inner(c, sums):
                sums = list(sums)
                for i in range(QB):
                    q = 1 + c * QB + i
                    sources = [even[k, q] if which == 0 else odd[o, q] for which in parts]
                    for j in range(PB):
                        weight = row(inv, k, b * PB + j, pl.ds(q, 1), slice(None))
                        for n, source in enumerate(sources):
                            sums[n * PB + j] = sums[n * PB + j] + weight * source
                return tuple(sums)

            sums = lax.fori_loop(0, (NP - 2) // QB, inner, (zero,) * (len(parts) * PB))
            for j in range(PB):
                p = b * PB + j
                for n, which in enumerate(parts):
                    if which == 0:
                        even_part[k, p] = sums[n * PB + j]
                    else:
                        odd_part[o, p] = sums[n * PB + j]
            return 0

        lax.fori_loop(0, NP // PB, block, 0)

    def factor(k):
        def influence(s, i):
            return row(even_slopes, k, s, 2, slice(i, i + 1), slice(None))

        last = NS - 2
        lower = [influence(s, 2) for s in range(NS - 1)]
        middle = [influence(s, 3) - influence(s + 1, 0) for s in range(NS - 1)]
        upper = [-influence(s + 1, 1) for s in range(NS - 1)]
        ratio = [zero] * (NS - 1)
        scale = [zero] * (NS - 1)
        for s in range(3):
            scale[s] = 1.0 / (middle[s] - lower[s] * ratio[s - 1] if s else middle[s])
            ratio[s] = upper[s] * scale[s]
            r = last - s
            scale[r] = 1.0 / (middle[r] - upper[r] * ratio[r + 1] if s else middle[r])
            ratio[r] = lower[r] * scale[r]
        scale[3] = 1.0 / ((middle[3] - lower[3] * ratio[2]) - upper[3] * ratio[4])
        for s in range(NS - 1):
            factors[0, s] = lower[s]
            factors[1, s] = upper[s]
            factors[2, s] = ratio[s]
            factors[3, s] = scale[s]

    def interface(k, which):
        slopes = even_slopes.at[k] if which == 0 else odd_slopes.at[half(k)]
        last = NS - 2
        right = [slopes[s + 1, 0] - slopes[s, 1] for s in range(NS - 1)]
        lower = [factors[0, s] for s in range(NS - 1)]
        upper = [factors[1, s] for s in range(NS - 1)]
        ratio = [factors[2, s] for s in range(NS - 1)]
        scale = [factors[3, s] for s in range(NS - 1)]
        reduced = [zero] * (NS - 1)
        for s in range(3):
            r = last - s
            reduced[s] = (right[s] - lower[s] * reduced[s - 1] if s else right[s]) * scale[s]
            reduced[r] = (right[r] - upper[r] * reduced[r + 1] if s else right[r]) * scale[r]
        found = [zero] * (NS - 1)
        found[3] = ((right[3] - lower[3] * reduced[2]) - upper[3] * reduced[4]) * scale[3]
        for s in (2, 1, 0):
            found[s] = reduced[s] - ratio[s] * found[s + 1]
            found[last - s] = reduced[last - s] - ratio[last - s] * found[last - s - 1]
        values[which, 0] = zero
        values[which, NS] = zero
        for s in range(NS - 1):
            values[which, s + 1] = found[s]
        return values[which, sub], values[which, sub + 1]

    def finish_step(k):
        even_all(k).wait()
        factor(k)
        below, above = interface(k, 0)
        if k == 0:
            own_ends[0] = below
            own_ends[1] = above
            start(end_copies())
            far_ends[me, 0] = below
            far_ends[me, 1] = above
        else:
            correct_even(k, below, above)
        if has_odd(k):
            correct_odd(k)

    def correct_even(k, below, above):
        t = STEPS[k][1]
        u = half(k)
        position = lane + t * 128
        even_kept = position >= even_mode

        def block(b, _):
            for i in range(FB):
                p = b * FB + i
                first, final = ends(k, p)
                field = (even_part[k, p] + below * first) + above * final
                if not has_odd(k):
                    field = jnp.where(even_kept, field, odd_flip[u, p])
                sent[k, p] = field
            return 0

        lax.fori_loop(0, NP // FB, block, 0)
        packed[k, me] = sent[k, pl.ds(me * 4, 4)]
        start(field_copies(k))

    def correct_odd(k):
        t = STEPS[k][1]
        u = half(k)
        odd_all(k).wait()
        below, above = interface(k, 1)
        meets = lane + (3 - t) * 128 == even_mode

        def block(b, _):
            for a in range(FB // 4):
                last = zero
                for i in range(4):
                    p = b * FB + a * 4 + i
                    first, final = ends(k, p)
                    other = flip_lanes((odd_part[u, p] + below * first) + above * final)
                    odd_flip[u, p] = other
                    value = jnp.sum(jnp.where(meets, other, 0.0), axis=1, keepdims=True)
                    last = jnp.where(lane == sublane + i * 8, value, last)
                last_rows[u, b * (FB // 4) + a] = jnp.sum(last, axis=0, keepdims=True)
            return 0

        lax.fori_loop(0, NP // FB, block, 0)
        extras[u, me] = last_rows[u, me]
        start(last_copies(u))

    def field_source(k):
        return even_part.at[k] if k == 0 else sent.at[k]

    def end_copies():
        return [
            pltpu.make_async_remote_copy(
                own_ends, far_ends.at[me], end_send, end_recv, device_id={"ma": other}, device_id_type=MESH
            )
            for other in peers
        ]

    def end_all():
        most = far_ends.at[pl.ds(0, NM - 1)]
        return pltpu.make_async_remote_copy(
            most, most, end_send, end_recv, device_id={"ma": peers[0]}, device_id_type=MESH
        )

    def field_copies(k):
        return [
            pltpu.make_async_remote_copy(
                field_source(k).at[pl.ds(other * 4, 4)], packed.at[k, me], field_send.at[k], field_recv.at[k],
                device_id={"ma": other}, device_id_type=MESH,
            )
            for other in peers
        ]

    def field_all(k):
        return pltpu.make_async_remote_copy(
            field_source(k).at[pl.ds(0, NP - 4)], packed.at[k, pl.ds(0, NM - 1)], field_send.at[k], field_recv.at[k],
            device_id={"ma": peers[0]}, device_id_type=MESH,
        )

    def last_copies(u):
        return [
            pltpu.make_async_remote_copy(
                last_rows.at[u, other], extras.at[u, me], last_send.at[u], last_recv.at[u],
                device_id={"ma": other}, device_id_type=MESH,
            )
            for other in peers
        ]

    def last_all(u):
        return pltpu.make_async_remote_copy(
            last_rows.at[u, pl.ds(0, NM - 1)], extras.at[u, pl.ds(0, NM - 1)], last_send.at[u], last_recv.at[u],
            device_id={"ma": peers[0]}, device_id_type=MESH,
        )

    def mode_copies():
        return [
            pltpu.make_async_remote_copy(
                own_modes, modes.at[me], mode_send, mode_recv, device_id={"ma": other}, device_id_type=MESH
            )
            for other in peers
        ]

    def mode_all():
        most = modes.at[pl.ds(0, NM - 1)]
        return pltpu.make_async_remote_copy(
            most, most, mode_send, mode_recv, device_id={"ma": peers[0]}, device_id_type=MESH
        )

    def unpack(u):
        f, t = STEPS[2 * u]
        near = 3 - t
        is_odd = lax.rem(sublane, 2) == 1
        pick = [sublane // 2, sublane // 2 + 4]

        corrections = [ends(0, me * 4 + p) for p in range(4)] if u == 0 else None

        def spread(value, c):
            return jnp.take_along_axis(value, pick[c], axis=0)

        def block(b, _):
            for i in range(8):
                a = b * 8 + i
                mode = modes[a].astype(jnp.int32)
                even_kept = lane + near * 128 >= mode
                odd_at = lane + t * 128 + mode
                rows = pl.ds(pl.multiple_of(a * 8, 8), 8)
                row_extras = row(extras, u, a)
                for p in range(4):
                    merged = packed[2 * u + 1, a, p]
                    extra = jnp.take_along_axis(row_extras, sublane + p * 8, axis=1)
                    other = jnp.where(odd_at > 511, flip_lanes(merged), jnp.where(odd_at == 511, extra, 0.0))
                    far = packed[2 * u, a, p]
                    if u == 0:
                        far = (far + far_ends[a, 0] * corrections[p][0]) + far_ends[a, 1] * corrections[p][1]
                    close = jnp.where(even_kept, merged, 0.0)
                    for c in range(2):
                        out[f, p, c, rows, t * 128 : t * 128 + 128] = jnp.where(
                            is_odd, spread(other, c), spread(far, c)
                        )
                        out[f, p, c, rows, near * 128 : near * 128 + 128] = jnp.where(is_odd, 0.0, spread(close, c))
            return 0

        lax.fori_loop(0, NM // 8, block, 0)

    def greet():
        pl.semaphore_wait(barrier, len(subs) + len(peers))
        modes[me] = own_modes[...]

    for item in ORDER:
        k = int(item[1])
        if item[0] == "S":
            slope_step(k, greet if k == 0 else None)
            if k == 0:
                start(mode_copies())
        elif item[0] == "R":
            start(field_copies(k))
            packed[k, me] = even_part[k, pl.ds(me * 4, 4)]
        elif item[0] == "F":
            finish_step(k)
        else:
            particular_step(k, {"E": (0,), "O": (1,), "P": (0, 1) if has_odd(k) else (0,)}[item[0]])

    mode_all().wait()
    end_all().wait()
    for u in range(NSTEP // 2):
        field_all(2 * u).wait()
        field_all(2 * u + 1).wait()
        last_all(u).wait()
        unpack(u)


def body(forcing, slot_wavenumber, inverse, edge_weights):
    vmem = pl.BlockSpec(memory_space=pltpu.VMEM)
    anywhere = pl.BlockSpec(memory_space=pl.ANY)
    dma = pltpu.SemaphoreType.DMA
    units = NSTEP // 2
    return pl.pallas_call(
        solve_kernel,
        out_shape=jax.ShapeDtypeStruct((2, 4, 2, 128, 512), F32),
        in_specs=[anywhere] * 4,
        out_specs=vmem,
        scratch_shapes=[
            pltpu.SMEM((8,), jnp.int32),
            pltpu.SMEM((1, 2, NP), F32),
            pltpu.VMEM((NSTEP, NP, NP, 128), F32),
            pltpu.VMEM((NSTEP, NP, 16, 128), F32),
            pltpu.VMEM((NSTEP, NP, 8, 128), F32),
            pltpu.VMEM((units, NP, 8, 128), F32),
            pltpu.VMEM((NSTEP, NP, 8, 128), F32),
            pltpu.VMEM((units, NP, 8, 128), F32),
            pltpu.VMEM((units, NP, 8, 128), F32),
            pltpu.VMEM((NSTEP, NP, 8, 128), F32),
            pltpu.VMEM((NSTEP, NM, 4, 8, 128), F32),
            pltpu.VMEM((2, NP, 128), F32),
            pltpu.VMEM((2, NP, 8, 128), F32),
            pltpu.VMEM((NSTEP, NS, 3, 8, 128), F32),
            pltpu.VMEM((units, NS, 2, 8, 128), F32),
            pltpu.VMEM((4, NS - 1, 8, 128), F32),
            pltpu.VMEM((2, NS + 1, 8, 128), F32),
            pltpu.VMEM((units, NM, 1, 128), F32),
            pltpu.VMEM((units, NM, 1, 128), F32),
            pltpu.VMEM((8, 128), F32),
            pltpu.VMEM((NM, 8, 128), F32),
            pltpu.VMEM((2, 8, 128), F32),
            pltpu.VMEM((NM, 2, 8, 128), F32),
            dma((2,)),
            dma((NSTEP,)),
            dma((NSTEP,)),
            dma((NSTEP,)),
            dma((NSTEP,)),
            dma((units,)),
            dma((units,)),
            dma((NSTEP,)),
            dma((NSTEP,)),
            dma((units,)),
            dma((units,)),
            dma,
            dma,
            dma,
            dma,
        ],
        compiler_params=pltpu.CompilerParams(
            collective_id=0, has_side_effects=True, vmem_limit_bytes=48 * 1024 * 1024
        ),
        name="solve_and_exchange",
    )(
        forcing.reshape(2, NP, 16, 512),
        pltpu.with_memory_space_constraint(slot_wavenumber, pltpu.HBM),
        pltpu.with_memory_space_constraint(edge_weights, pltpu.HBM),
        inverse[0],
    )


def solution(mesh):
    return jax.shard_map(
        body,
        mesh=mesh,
        in_specs=(
            P(None, "sub", None, "ma", None),
            P("ma"),
            P("sub", None, None, None, None),
            P("sub", None, None),
        ),
        out_specs=P(None, ("sub", "ma"), None, None, None),
        check_vma=False,
    )
```

```python
import jax
import jax.numpy as jnp
from jax import lax
from jax.experimental import pallas as pl
from jax.experimental.pallas import tpu as pltpu
from jax.sharding import PartitionSpec as P

MESH = pl.DeviceIdType.MESH
F32 = jnp.float32
NP = 64
NS = 8
NM = 16
TILES = (2, 1, 3, 0)
STEPS = tuple((f, t) for f in range(2) for t in TILES)
NSTEP = len(STEPS)
AHEAD = 3
PB = 8
QB = 31
FB = 32
ORDER = (
    "S0", "E0", "R0", "S1", "O0", "S2", "P1", "F0", "G0", "F1", "S3", "P2", "F2", "G2", "S4", "P3",
    "F3", "S5", "P4", "F4", "G4", "S6", "P5", "F5", "S7", "P6", "F6", "G6", "P7", "F7",
)


def has_odd(k):
    return STEPS[k][1] >= 2


def half(k):
    return k // 2


def iota(dim):
    return lax.broadcasted_iota(jnp.int32, (8, 128), dim)


def row(ref, *at):
    return jnp.broadcast_to(ref[at], (8, 128))


def flip_lanes(x):
    return jnp.take_along_axis(x, 127 - iota(1), axis=1)


def solve_kernel(
    forcing, slot_hbm, edge_hbm, inverse, out,
    slots, edges, inv, raw, even, odd, even_part, odd_part, odd_flip, sent, packed, weights, splats,
    even_slopes, odd_slopes, factors, values, last_rows, extras, own_modes, modes, own_ends, far_ends,
    small_sem, inv_sem, raw_sem, even_send, even_recv, odd_send, odd_recv,
    field_send, field_recv, last_send, last_recv, mode_send, mode_recv, end_send, end_recv,
):
    sub = lax.axis_index("sub")
    me = lax.axis_index("ma")
    y, x = me // 4, lax.rem(me, 4)
    chip, core = sub // 2, lax.rem(sub, 2)
    subs = []
    for dz in (2, 1, 3, 0):
        for dc in (0, 1):
            if dz or dc:
                subs.append(lax.rem(chip + dz, 4) * 2 + lax.rem(core + dc, 2))
    peers = []
    for dy in (2, 1, 3, 0):
        for dx in (2, 1, 3, 0):
            if dy or dx:
                peers.append(lax.rem(y + dy, 4) * 4 + lax.rem(x + dx, 4))

    def load(k):
        f, t = STEPS[k]
        lanes = pl.ds(t * 128, 128)
        return (
            pltpu.make_async_copy(forcing.at[f, :, :, lanes], raw.at[k], raw_sem.at[k]),
            pltpu.make_async_copy(inverse.at[f, :, :, lanes], inv.at[k], inv_sem.at[k]),
        )

    def start(copies):
        for copy in copies:
            copy.start()

    barrier = pltpu.get_barrier_semaphore()
    for other in subs:
        pl.semaphore_signal(barrier, inc=1, device_id={"sub": other}, device_id_type=MESH)
    for other in peers:
        pl.semaphore_signal(barrier, inc=1, device_id={"ma": other}, device_id_type=MESH)
    small = (
        pltpu.make_async_copy(slot_hbm, slots, small_sem.at[0]),
        pltpu.make_async_copy(edge_hbm, edges, small_sem.at[1]),
    )
    start(small)
    start(load(0))
    for k in range(1, AHEAD):
        start(load(k))

    for copy in small:
        copy.wait()
    zero = jnp.zeros((8, 128), F32)
    lane = iota(1)
    sublane = iota(0)
    pair = lax.rem(sublane, 4)
    even_mode = jnp.zeros((8, 128), jnp.int32)
    odd_mode = jnp.zeros((8, 128), jnp.int32)
    for j in range(4):
        even_mode = jnp.where(pair == j, slots[2 * j], even_mode)
        odd_mode = jnp.where(pair == j, slots[2 * j + 1], odd_mode)
    own_modes[...] = even_mode.astype(F32)
    for e in range(2):
        for p in range(NP):
            splats[e, p] = jnp.full((8, 128), edges[0, e, p], F32)

    def prepare(k, which):
        f, t = STEPS[k]
        kept = lane + t * 128 >= (even_mode if which == 0 else odd_mode)
        target = even.at[k] if which == 0 else odd.at[half(k)]

        def block(b, _):
            for i in range(8):
                q = b * 8 + i
                target[q] = jnp.where(kept, raw[k, q, pl.ds(which, 8, stride=2), :], zero)
            return 0

        lax.fori_loop(0, NP // 8, block, 0)
        target[0] = zero
        target[NP - 1] = zero

    def weigh(k):
        def block(b, _):
            def inner(c, sums):
                sums = list(sums)
                for j in range(16):
                    p = c * 16 + j
                    low, top = splats[0, p], splats[1, p]
                    for i in range(4):
                        tile = inv[k, p, pl.ds(pl.multiple_of(b * 32 + i * 8, 8), 8), :]
                        sums[i] = sums[i] + low * tile
                        sums[4 + i] = sums[4 + i] + top * tile
                return tuple(sums)

            sums = lax.fori_loop(0, NP // 16, inner, (zero,) * 8)
            for i in range(4):
                rows = pl.ds(pl.multiple_of(b * 32 + i * 8, 8), 8)
                weights[0, rows, :] = sums[i]
                weights[1, rows, :] = sums[4 + i]
            return 0

        lax.fori_loop(0, NP // 32, block, 0)

    def slope_sums(k, which):
        source = even.at[k] if which == 0 else odd.at[half(k)]
        def block(b, sums):
            sums = list(sums)
            for i in range(8):
                q = b * 8 + i
                for e in range(2):
                    at = 2 * e + i % 2
                    sums[at] = sums[at] + row(weights, e, pl.ds(q, 1), slice(None)) * source[q]
            return tuple(sums)

        sums = lax.fori_loop(0, NP // 8, block, (zero,) * 4)
        return sums[0] + sums[1], sums[2] + sums[3]

    def even_copies(k):
        here = even_slopes.at[k, sub]
        return [
            pltpu.make_async_remote_copy(
                here, here, even_send.at[k], even_recv.at[k], device_id={"sub": other}, device_id_type=MESH
            )
            for other in subs
        ]

    def odd_copies(k):
        here = odd_slopes.at[half(k), sub]
        return [
            pltpu.make_async_remote_copy(
                here, here, odd_send.at[half(k)], odd_recv.at[half(k)], device_id={"sub": other}, device_id_type=MESH
            )
            for other in subs
        ]

    def even_all(k):
        most = even_slopes.at[k, pl.ds(0, NS - 1)]
        return pltpu.make_async_remote_copy(
            most, most, even_send.at[k], even_recv.at[k], device_id={"sub": subs[0]}, device_id_type=MESH
        )

    def odd_all(k):
        most = odd_slopes.at[half(k), pl.ds(0, NS - 1)]
        return pltpu.make_async_remote_copy(
            most, most, odd_send.at[half(k)], odd_recv.at[half(k)], device_id={"sub": subs[0]}, device_id_type=MESH
        )

    def slope_step(k, before_send=None):
        source_copy, inverse_copy = load(k)
        source_copy.wait()
        prepare(k, 0)
        if has_odd(k):
            prepare(k, 1)
        inverse_copy.wait()
        if k + AHEAD < NSTEP:
            start(load(k + AHEAD))
        weigh(k)
        low, top = slope_sums(k, 0)
        even_slopes[k, sub, 0] = low
        even_slopes[k, sub, 1] = top
        for e in range(2):
            for i, q in enumerate((0, NP - 1)):
                even_slopes[k, sub, 2, 2 * e + i : 2 * e + i + 1, :] = weights[e, q : q + 1, :]
        if before_send is not None:
            before_send()
        start(even_copies(k))
        if has_odd(k):
            low, top = slope_sums(k, 1)
            odd_slopes[half(k), sub, 0] = low
            odd_slopes[half(k), sub, 1] = top
            start(odd_copies(k))

    def ends(k, p):
        return (
            row(inv, k, p, slice(0, 1), slice(None)),
            row(inv, k, p, slice(NP - 1, NP), slice(None)),
        )

    def particular_step(k, parts):
        o = half(k)

        def block(b, _):
            def inner(c, sums):
                sums = list(sums)
                for i in range(QB):
                    q = 1 + c * QB + i
                    sources = [even[k, q] if which == 0 else odd[o, q] for which in parts]
                    for j in range(PB):
                        weight = row(inv, k, b * PB + j, pl.ds(q, 1), slice(None))
                        for n, source in enumerate(sources):
                            sums[n * PB + j] = sums[n * PB + j] + weight * source
                return tuple(sums)

            sums = lax.fori_loop(0, (NP - 2) // QB, inner, (zero,) * (len(parts) * PB))
            for j in range(PB):
                p = b * PB + j
                for n, which in enumerate(parts):
                    if which == 0:
                        even_part[k, p] = sums[n * PB + j]
                    else:
                        odd_part[o, p] = sums[n * PB + j]
            return 0

        lax.fori_loop(0, NP // PB, block, 0)

    def factor(k):
        def influence(s, i):
            return row(even_slopes, k, s, 2, slice(i, i + 1), slice(None))

        last = NS - 2
        lower = [influence(s, 2) for s in range(NS - 1)]
        middle = [influence(s, 3) - influence(s + 1, 0) for s in range(NS - 1)]
        upper = [-influence(s + 1, 1) for s in range(NS - 1)]
        ratio = [zero] * (NS - 1)
        scale = [zero] * (NS - 1)
        for s in range(3):
            scale[s] = 1.0 / (middle[s] - lower[s] * ratio[s - 1] if s else middle[s])
            ratio[s] = upper[s] * scale[s]
            r = last - s
            scale[r] = 1.0 / (middle[r] - upper[r] * ratio[r + 1] if s else middle[r])
            ratio[r] = lower[r] * scale[r]
        scale[3] = 1.0 / ((middle[3] - lower[3] * ratio[2]) - upper[3] * ratio[4])
        for s in range(NS - 1):
            factors[0, s] = lower[s]
            factors[1, s] = upper[s]
            factors[2, s] = ratio[s]
            factors[3, s] = scale[s]

    def interface(k, which):
        slopes = even_slopes.at[k] if which == 0 else odd_slopes.at[half(k)]
        last = NS - 2
        right = [slopes[s + 1, 0] - slopes[s, 1] for s in range(NS - 1)]
        lower = [factors[0, s] for s in range(NS - 1)]
        upper = [factors[1, s] for s in range(NS - 1)]
        ratio = [factors[2, s] for s in range(NS - 1)]
        scale = [factors[3, s] for s in range(NS - 1)]
        reduced = [zero] * (NS - 1)
        for s in range(3):
            r = last - s
            reduced[s] = (right[s] - lower[s] * reduced[s - 1] if s else right[s]) * scale[s]
            reduced[r] = (right[r] - upper[r] * reduced[r + 1] if s else right[r]) * scale[r]
        found = [zero] * (NS - 1)
        found[3] = ((right[3] - lower[3] * reduced[2]) - upper[3] * reduced[4]) * scale[3]
        for s in (2, 1, 0):
            found[s] = reduced[s] - ratio[s] * found[s + 1]
            found[last - s] = reduced[last - s] - ratio[last - s] * found[last - s - 1]
        values[which, 0] = zero
        values[which, NS] = zero
        for s in range(NS - 1):
            values[which, s + 1] = found[s]
        return values[which, sub], values[which, sub + 1]

    def finish_step(k):
        even_all(k).wait()
        factor(k)
        below, above = interface(k, 0)
        if k == 0:
            own_ends[0] = below
            own_ends[1] = above
            start(end_copies())
            far_ends[me, 0] = below
            far_ends[me, 1] = above
        else:
            correct_even(k, below, above)

    def correct_even(k, below, above):
        t = STEPS[k][1]
        u = half(k)
        position = lane + t * 128
        even_kept = position >= even_mode

        def block(b, _):
            for i in range(FB):
                p = b * FB + i
                first, final = ends(k, p)
                field = (even_part[k, p] + below * first) + above * final
                if not has_odd(k):
                    field = jnp.where(even_kept, field, odd_flip[u, p])
                sent[k, p] = field
            return 0

        lax.fori_loop(0, NP // FB, block, 0)
        packed[k, me] = sent[k, pl.ds(me * 4, 4)]
        start(field_copies(k))

    def correct_odd(k):
        t = STEPS[k][1]
        u = half(k)
        odd_all(k).wait()
        below, above = interface(k, 1)
        meets = lane + t * 128 == odd_mode

        def block(b, _):
            for a in range(FB // 4):
                last = zero
                for i in range(4):
                    p = b * FB + a * 4 + i
                    first, final = ends(k, p)
                    other = (odd_part[u, p] + below * first) + above * final
                    odd_flip[u, p] = flip_lanes(other)
                    value = jnp.sum(jnp.where(meets, other, 0.0), axis=1, keepdims=True)
                    last = jnp.where(lane == sublane + i * 8, value, last)
                last_rows[u, b * (FB // 4) + a] = jnp.sum(last, axis=0, keepdims=True)
            return 0

        lax.fori_loop(0, NP // FB, block, 0)
        extras[u, me] = last_rows[u, me]
        start(last_copies(u))

    def field_source(k):
        return even_part.at[k] if k == 0 else sent.at[k]

    def end_copies():
        return [
            pltpu.make_async_remote_copy(
                own_ends, far_ends.at[me], end_send, end_recv, device_id={"ma": other}, device_id_type=MESH
            )
            for other in peers
        ]

    def end_all():
        most = far_ends.at[pl.ds(0, NM - 1)]
        return pltpu.make_async_remote_copy(
            most, most, end_send, end_recv, device_id={"ma": peers[0]}, device_id_type=MESH
        )

    def field_copies(k):
        return [
            pltpu.make_async_remote_copy(
                field_source(k).at[pl.ds(other * 4, 4)], packed.at[k, me], field_send.at[k], field_recv.at[k],
                device_id={"ma": other}, device_id_type=MESH,
            )
            for other in peers
        ]

    def field_all(k):
        return pltpu.make_async_remote_copy(
            field_source(k).at[pl.ds(0, NP - 4)], packed.at[k, pl.ds(0, NM - 1)], field_send.at[k], field_recv.at[k],
            device_id={"ma": peers[0]}, device_id_type=MESH,
        )

    def last_copies(u):
        return [
            pltpu.make_async_remote_copy(
                last_rows.at[u, other], extras.at[u, me], last_send.at[u], last_recv.at[u],
                device_id={"ma": other}, device_id_type=MESH,
            )
            for other in peers
        ]

    def last_all(u):
        return pltpu.make_async_remote_copy(
            last_rows.at[u, pl.ds(0, NM - 1)], extras.at[u, pl.ds(0, NM - 1)], last_send.at[u], last_recv.at[u],
            device_id={"ma": peers[0]}, device_id_type=MESH,
        )

    def mode_copies():
        return [
            pltpu.make_async_remote_copy(
                own_modes, modes.at[me], mode_send, mode_recv, device_id={"ma": other}, device_id_type=MESH
            )
            for other in peers
        ]

    def mode_all():
        most = modes.at[pl.ds(0, NM - 1)]
        return pltpu.make_async_remote_copy(
            most, most, mode_send, mode_recv, device_id={"ma": peers[0]}, device_id_type=MESH
        )

    def unpack(u):
        f, t = STEPS[2 * u]
        near = 3 - t
        is_odd = lax.rem(sublane, 2) == 1
        pick = [sublane // 2, sublane // 2 + 4]

        corrections = [ends(0, me * 4 + p) for p in range(4)] if u == 0 else None

        def spread(value, c):
            return jnp.take_along_axis(value, pick[c], axis=0)

        def block(b, _):
            for i in range(16):
                a = b * 16 + i
                mode = modes[a].astype(jnp.int32)
                even_kept = lane + near * 128 >= mode
                odd_at = lane + t * 128 + mode
                rows = pl.ds(pl.multiple_of(a * 8, 8), 8)
                row_extras = row(extras, u, a)
                for p in range(4):
                    merged = packed[2 * u + 1, a, p]
                    extra = jnp.take_along_axis(row_extras, sublane + p * 8, axis=1)
                    other = jnp.where(odd_at > 511, flip_lanes(merged), jnp.where(odd_at == 511, extra, 0.0))
                    far = packed[2 * u, a, p]
                    if u == 0:
                        far = (far + far_ends[a, 0] * corrections[p][0]) + far_ends[a, 1] * corrections[p][1]
                    close = jnp.where(even_kept, merged, 0.0)
                    for c in range(2):
                        out[f, p, c, rows, t * 128 : t * 128 + 128] = jnp.where(
                            is_odd, spread(other, c), spread(far, c)
                        )
                        out[f, p, c, rows, near * 128 : near * 128 + 128] = jnp.where(is_odd, 0.0, spread(close, c))
            return 0

        lax.fori_loop(0, NM // 16, block, 0)

    def greet():
        pl.semaphore_wait(barrier, len(subs) + len(peers))
        modes[me] = own_modes[...]

    for item in ORDER:
        k = int(item[1])
        if item[0] == "S":
            slope_step(k, greet if k == 0 else None)
            if k == 0:
                start(mode_copies())
        elif item[0] == "R":
            start(field_copies(k))
            packed[k, me] = even_part[k, pl.ds(me * 4, 4)]
        elif item[0] == "F":
            finish_step(k)
        elif item[0] == "G":
            correct_odd(k)
        else:
            particular_step(k, {"E": (0,), "O": (1,), "P": (0, 1) if has_odd(k) else (0,)}[item[0]])

    mode_all().wait()
    end_all().wait()
    for u in range(NSTEP // 2):
        field_all(2 * u).wait()
        field_all(2 * u + 1).wait()
        last_all(u).wait()
        unpack(u)


def body(forcing, slot_wavenumber, inverse, edge_weights):
    vmem = pl.BlockSpec(memory_space=pltpu.VMEM)
    anywhere = pl.BlockSpec(memory_space=pl.ANY)
    dma = pltpu.SemaphoreType.DMA
    units = NSTEP // 2
    return pl.pallas_call(
        solve_kernel,
        out_shape=jax.ShapeDtypeStruct((2, 4, 2, 128, 512), F32),
        in_specs=[anywhere] * 4,
        out_specs=vmem,
        scratch_shapes=[
            pltpu.SMEM((8,), jnp.int32),
            pltpu.SMEM((1, 2, NP), F32),
            pltpu.VMEM((NSTEP, NP, NP, 128), F32),
            pltpu.VMEM((NSTEP, NP, 16, 128), F32),
            pltpu.VMEM((NSTEP, NP, 8, 128), F32),
            pltpu.VMEM((units, NP, 8, 128), F32),
            pltpu.VMEM((NSTEP, NP, 8, 128), F32),
            pltpu.VMEM((units, NP, 8, 128), F32),
            pltpu.VMEM((units, NP, 8, 128), F32),
            pltpu.VMEM((NSTEP, NP, 8, 128), F32),
            pltpu.VMEM((NSTEP, NM, 4, 8, 128), F32),
            pltpu.VMEM((2, NP, 128), F32),
            pltpu.VMEM((2, NP, 8, 128), F32),
            pltpu.VMEM((NSTEP, NS, 3, 8, 128), F32),
            pltpu.VMEM((units, NS, 2, 8, 128), F32),
            pltpu.VMEM((4, NS - 1, 8, 128), F32),
            pltpu.VMEM((2, NS + 1, 8, 128), F32),
            pltpu.VMEM((units, NM, 1, 128), F32),
            pltpu.VMEM((units, NM, 1, 128), F32),
            pltpu.VMEM((8, 128), F32),
            pltpu.VMEM((NM, 8, 128), F32),
            pltpu.VMEM((2, 8, 128), F32),
            pltpu.VMEM((NM, 2, 8, 128), F32),
            dma((2,)),
            dma((NSTEP,)),
            dma((NSTEP,)),
            dma((NSTEP,)),
            dma((NSTEP,)),
            dma((units,)),
            dma((units,)),
            dma((NSTEP,)),
            dma((NSTEP,)),
            dma((units,)),
            dma((units,)),
            dma,
            dma,
            dma,
            dma,
        ],
        compiler_params=pltpu.CompilerParams(
            collective_id=0, has_side_effects=True, vmem_limit_bytes=48 * 1024 * 1024
        ),
        name="solve_and_exchange",
    )(
        forcing.reshape(2, NP, 16, 512),
        pltpu.with_memory_space_constraint(slot_wavenumber, pltpu.HBM),
        pltpu.with_memory_space_constraint(edge_weights, pltpu.HBM),
        inverse[0],
    )


def solution(mesh):
    return jax.shard_map(
        body,
        mesh=mesh,
        in_specs=(
            P(None, "sub", None, "ma", None),
            P("ma"),
            P("sub", None, None, None, None),
            P("sub", None, None),
        ),
        out_specs=P(None, ("sub", "ma"), None, None, None),
        check_vma=False,
    )
```
